32 devices in a mesh: group: 2 (over core), dp: 4 (over y, x), mp: 4 (over z).
Axes of the slice: x: 2, y: 2, z: 4, core: 2. Of those that a mesh axis runs over, the one named last changes fastest.
Arguments:
- x_arrive: bfloat16 [16, 256, 1152], P(('group', 'dp')), may hold values from -6 to 6
- cond_first: int32 [8], P(('group', 'dp')), may hold values 0 or 1
- labels: int32 [8], P(('group', 'dp')), may hold values from 0 to 999
- step_ids: int32 [8], P(('group', 'dp')), may hold values from 0 to 999
- guidance: float32 [1], replicated, may hold values from 2 to 6
- time_table: bfloat16 [1000, 1152], P(None, 'mp'), may hold values from -6 to 6
- class_table: bfloat16 [1001, 1152], P(None, 'mp'), may hold values from -6 to 6
- ada_weight: bfloat16 [1152, 6912], P('mp', 'dp'), may hold values from -0.1875 to 0.1875
- final_ada: bfloat16 [1152, 2304], P('mp'), may hold values from -0.1875 to 0.1875
- qkv_weight: bfloat16 [3, 1152, 1152], P(None, 'dp', 'mp'), may hold values from -2 to 2
- proj_weight: bfloat16 [1152, 1152], P('mp', 'dp'), may hold values from -0.1875 to 0.1875
- fc1_weight: bfloat16 [1152, 4608], P('dp', 'mp'), may hold values from -0.1875 to 0.1875
- fc2_weight: bfloat16 [4608, 1152], P('mp', 'dp'), may hold values from -0.09375 to 0.09375
- out_weight: bfloat16 [1152, 16], replicated, may hold values from -0.1875 to 0.1875
Outputs:
- guided: float32 [8, 4096], P(('group', 'dp'), 'mp')
The draws below stay inside these ranges and needn't reach their ends.
All inputs are finite; a program needn't handle non-finite values. No bound on the sum of `cond_first` on one device may be relied on, other than what follows from the above.
Results may differ from the reference program's by a relative error of at most 0.025.
Values may be sent and summed in bfloat16 or wider, within the bound.
A program may use at most 64 MiB of HBM per device.

```python
import math
import jax
import jax.numpy as jnp
import numpy as np
from jax import lax

D = 1152
HEADS = 16
FF = 4608
CLASSES = 1000
STEPS = 1000
OUT = 16
TOK = 256
PAIRS = 8
BATCH = 16
N_MP = 4


def draw_qkv_weight(key, part):
    stacked = jax.random.normal(key, (3, D, D), jnp.float32) / math.sqrt(D)
    return jnp.clip(stacked, -2.0, 2.0).astype(jnp.bfloat16)


def plant(values, key, least, top_value):
    index_at = [jax.random.randint(jax.random.fold_in(key, axis), (), 0, length) for axis, length in enumerate(values.shape)]
    widest = values.shape.index(max(values.shape))
    beside = index_at[:widest] + [(index_at[widest] + 1) % values.shape[widest]] + index_at[widest + 1:]
    return values.at[tuple(index_at)].set(least).at[tuple(beside)].set(top_value)


def steps_of(rng, shape, pieces, smallest, high):
    level, own = 1.0, jax.random.fold_in(rng, 6)
    for dim, blocks in pieces:
        heights = jnp.exp(jax.random.uniform(jax.random.fold_in(own, dim), (blocks,), jnp.float32, smallest / len(pieces), high / len(pieces)))
        level = level * jnp.repeat(heights, shape[dim] // blocks).reshape([-1 if axis == dim else 1 for axis in range(len(shape))])
    return level


def rank_table(number_of, skew):
    loads = [(1 << 20) // math.isqrt(standing ** skew) + 1 for standing in range(1, number_of + 1)]
    scale = 1 + sum(loads) // (1 << 30)
    return np.cumsum(np.array([max(1, weight // scale) for weight in loads]))


def skewed_ids(own_key, shape, number_of, slope):
    grid = rank_table(number_of, slope)
    ticket = jax.random.randint(jax.random.fold_in(own_key, 1), shape, 0, int(grid[number_of - 1]))
    grade = jnp.searchsorted(jnp.asarray(grid, jnp.int32), ticket, side="right")
    return jax.random.permutation(jax.random.fold_in(own_key, 2), number_of)[grade].astype(jnp.int32)


def gaussian(key, shape, deviation, reach, cuts=(), held_as=jnp.bfloat16):
    result = jax.random.normal(key, shape, jnp.float32) * deviation
    if len(cuts) > 0:
        result = steps_of(key, shape, cuts, -0.22, 0.18) * result
    return jnp.clip(result, min=-reach, max=reach).astype(held_as)


def setup_inputs(seed: int = 0) -> dict:
    arg_keys = jax.random.split(jax.random.key(seed), 15)
    x_arrive = gaussian(arg_keys[0], (BATCH, TOK, D), 1.0, 6.0, ((0, 8),))
    cond_first = plant((jax.random.randint(arg_keys[1], (PAIRS,), 0, 2) < 1).astype(jnp.int32), jax.random.fold_in(arg_keys[1], 1), 0, 1)
    labels = plant(skewed_ids(arg_keys[2], (PAIRS,), CLASSES, 2), jax.random.fold_in(arg_keys[2], 3), 0, CLASSES - 1).astype(jnp.int32)
    step_ids = plant(jax.random.randint(arg_keys[3], (PAIRS,), 0, STEPS), jax.random.fold_in(arg_keys[3], 1), 0, STEPS - 1).astype(jnp.int32)
    guidance = jnp.clip(jax.random.uniform(arg_keys[4], (1,), jnp.float32, 2.0, 6.0), 2.0, 6.0)
    time_table = gaussian(arg_keys[5], (STEPS, D), 1.0, 6.0, ((1, 4),))
    class_table = gaussian(arg_keys[6], (CLASSES + 1, D), 1.0, 6.0, ((1, 4),))
    ada_weight = gaussian(arg_keys[7], (D, 6 * D), D ** -0.5, 0.1875, ((0, 4), (1, 4)))
    final_ada = gaussian(arg_keys[8], (D, 2 * D), D ** -0.5, 0.1875, ((0, 4),))
    qkv_weight = draw_qkv_weight(jax.random.fold_in(arg_keys[14], 71), 0)
    proj_weight = gaussian(arg_keys[10], (D, D), D ** -0.5, 0.1875, ((0, 4), (1, 4)))
    fc1_weight = gaussian(arg_keys[11], (D, FF), D ** -0.5, 0.1875, ((0, 4), (1, 4)))
    fc2_weight = gaussian(arg_keys[12], (FF, D), FF ** -0.5, 0.09375, ((0, 4), (1, 4)))
    out_weight = gaussian(arg_keys[13], (D, OUT), D ** -0.5, 0.1875)
    return dict(x_arrive=x_arrive, cond_first=cond_first, labels=labels, step_ids=step_ids, guidance=guidance, time_table=time_table, class_table=class_table, ada_weight=ada_weight, final_ada=final_ada, qkv_weight=qkv_weight, proj_weight=proj_weight, fc1_weight=fc1_weight, fc2_weight=fc2_weight, out_weight=out_weight)


def layer_norm(values):
    mean = lax.optimization_barrier(jnp.mean(values, axis=-1, keepdims=True))
    centred = values - mean
    spread = lax.optimization_barrier(jnp.mean(centred * centred, axis=-1, keepdims=True))
    return centred * lax.rsqrt(spread + 1e-06)

def reference(x_arrive, cond_first, labels, step_ids, guidance, time_table, class_table, ada_weight, final_ada, qkv_weight, proj_weight, fc1_weight, fc2_weight, out_weight):
    head_dim = D // HEADS
    rows_all = 2 * TOK
    pair_rows = x_arrive.reshape(PAIRS, 2, TOK, D)

    def one_pair(item):
        rows, flag, label, step = item
        first = flag == 1
        cond_rows = jnp.where(first, rows[0], rows[1])
        uncond_rows = jnp.where(first, rows[1], rows[0])
        images = jnp.stack([cond_rows, uncond_rows]).astype(jnp.float32)
        time_part = time_table[step].astype(jnp.float32)
        class_part = jnp.stack([class_table[label], class_table[CLASSES]]).astype(jnp.float32)
        emb = time_part[None, :] + class_part
        act = jax.nn.silu(emb).astype(jnp.bfloat16)
        mods = jnp.dot(act, ada_weight, preferred_element_type=jnp.float32)
        fmods = jnp.dot(act, final_ada, preferred_element_type=jnp.float32)
        shift_a, scale_a, gate_a, shift_m, scale_m, gate_m = jnp.split(mods, 6, axis=1)
        shift_f, scale_f = jnp.split(fmods, 2, axis=1)
        hidden = (layer_norm(images) * (1.0 + scale_a[:, None]) + shift_a[:, None]).astype(jnp.bfloat16)
        flat = hidden.reshape(rows_all, D)
        query = jnp.dot(flat, qkv_weight[0], preferred_element_type=jnp.float32).astype(jnp.bfloat16)
        keys = jnp.dot(flat, qkv_weight[1], preferred_element_type=jnp.float32).astype(jnp.bfloat16)
        values = jnp.dot(flat, qkv_weight[2], preferred_element_type=jnp.float32).astype(jnp.bfloat16)
        query = query.reshape(2, TOK, HEADS, head_dim).astype(jnp.float32)
        keys = keys.reshape(2, TOK, HEADS, head_dim).astype(jnp.float32)
        values = values.reshape(2, TOK, HEADS, head_dim).astype(jnp.float32)
        scores = jnp.einsum('bqhe,bkhe->bhqk', query, keys) * head_dim ** (-0.5)
        probs = jax.nn.softmax(scores, axis=-1).astype(jnp.bfloat16)
        mixed = jnp.einsum('bhqk,bkhe->bqhe', probs.astype(jnp.float32), values).astype(jnp.bfloat16)
        mixed = mixed.reshape(rows_all, N_MP, D // N_MP).astype(jnp.float32)
        proj_groups = proj_weight.reshape(N_MP, D // N_MP, D).astype(jnp.float32)
        attn_parts = jnp.einsum('rgc,gcd->grd', mixed, proj_groups).astype(jnp.bfloat16)
        attn = lax.optimization_barrier(jnp.sum(attn_parts.astype(jnp.float32), axis=0)).reshape(2, TOK, D)
        first_sum = images + gate_a[:, None] * attn
        hidden_two = (layer_norm(first_sum) * (1.0 + scale_m[:, None]) + shift_m[:, None]).astype(jnp.bfloat16)
        up = jnp.dot(hidden_two.reshape(rows_all, D), fc1_weight, preferred_element_type=jnp.float32)
        gelu_h = jax.nn.gelu(up, approximate=True).astype(jnp.bfloat16)
        gelu_groups = gelu_h.reshape(rows_all, N_MP, FF // N_MP).astype(jnp.float32)
        down_groups = fc2_weight.reshape(N_MP, FF // N_MP, D).astype(jnp.float32)
        mlp_parts = jnp.einsum('rgc,gcd->grd', gelu_groups, down_groups).astype(jnp.bfloat16)
        mlp = lax.optimization_barrier(jnp.sum(mlp_parts.astype(jnp.float32), axis=0)).reshape(2, TOK, D)
        second_sum = first_sum + gate_m[:, None] * mlp
        fin = (layer_norm(second_sum) * (1.0 + scale_f[:, None]) + shift_f[:, None]).astype(jnp.bfloat16)
        noise = jnp.dot(fin.reshape(rows_all, D), out_weight, preferred_element_type=jnp.float32)
        noise = noise.reshape(2, TOK * OUT)
        return noise[1] + guidance[0] * (noise[0] - noise[1])
    return lax.map(one_pair, (pair_rows, cond_first, labels, step_ids))
```

```python
import jax
import jax.numpy as jnp
from jax import lax
from jax.experimental import pallas as pl
from jax.experimental.pallas import tpu as pltpu
from jax.sharding import PartitionSpec as P
import functools

HEADS = 16
CLASSES = 1000


def layer_norm(values):
    mean = jnp.mean(values, axis=-1, keepdims=True)
    centred = values - mean
    spread = jnp.mean(centred * centred, axis=-1, keepdims=True)
    return centred * lax.rsqrt(spread + 1e-06)


def on_device(
    x_arrive,
    cond_first,
    labels,
    step_ids,
    guidance,
    time_table,
    class_table,
    ada_weight,
    final_ada,
    qkv_weight,
    proj_weight,
    fc1_weight,
    fc2_weight,
    out_weight,
):
    pair_count = labels.shape[0]
    tokens = x_arrive.shape[1]
    width = x_arrive.shape[2]
    image_count = 2 * pair_count
    row_count = image_count * tokens
    split_rows = x_arrive.reshape(pair_count, 2, tokens, width)
    first = (cond_first == 1)[:, None, None]
    cond_rows = jnp.where(first, split_rows[:, 0], split_rows[:, 1])
    uncond_rows = jnp.where(first, split_rows[:, 1], split_rows[:, 0])
    x_sides = jnp.stack([cond_rows, uncond_rows])
    time_part = jnp.take(time_table, step_ids, axis=0).astype(jnp.float32)
    class_part = jnp.take(class_table, labels, axis=0).astype(jnp.float32)
    null_part = class_table[CLASSES].astype(jnp.float32)[None, :]
    emb_sides = time_part[None] + jnp.stack([class_part, null_part])
    act_sides = jax.nn.silu(emb_sides).astype(jnp.bfloat16)
    images, acts = (
        lax.all_to_all(x_sides, "group", split_axis=0, concat_axis=0, tiled=True),
        lax.all_to_all(act_sides, "group", split_axis=0, concat_axis=0, tiled=True),
    )
    images = images.reshape(image_count, tokens, width)
    acts = acts.reshape(image_count, act_sides.shape[2])
    partial_final = jnp.dot(acts, final_ada, preferred_element_type=jnp.float32)
    every_act = lax.all_gather(acts, "dp", axis=0, tiled=True)
    column_part = jnp.dot(every_act, ada_weight, preferred_element_type=jnp.float32)
    summed, fmods = (
        lax.psum(column_part.astype(jnp.bfloat16), "mp").astype(jnp.float32),
        lax.psum(partial_final.astype(jnp.bfloat16), "mp").astype(jnp.float32),
    )
    mods = lax.all_to_all(
        summed.astype(jnp.bfloat16), "dp", split_axis=0, concat_axis=1, tiled=True
    ).astype(summed.dtype)
    shift_a, scale_a, gate_a, shift_m, scale_m, gate_m = jnp.split(mods, 6, axis=1)
    shift_f, scale_f = jnp.split(fmods, 2, axis=1)
    images_f = images.astype(jnp.float32)
    hidden = (layer_norm(images_f) * (1.0 + scale_a[:, None]) + shift_a[:, None]).astype(
        jnp.bfloat16
    )
    hidden = hidden.reshape(row_count, width)
    quarter = qkv_weight.shape[2]
    head_dim = width // HEADS
    local_heads = quarter // head_dim
    columns = hidden
    qkv = jnp.einsum(
        "rd,kdc->krc",
        columns,
        lax.all_gather(qkv_weight, "dp", axis=1, tiled=True),
        preferred_element_type=jnp.float32,
    ).astype(jnp.bfloat16)
    query = qkv[0].reshape(image_count, tokens, local_heads, head_dim)
    keys = qkv[1].reshape(image_count, tokens, local_heads, head_dim)
    values = qkv[2].reshape(image_count, tokens, local_heads, head_dim)
    scores = jnp.einsum(
        "bqhe,bkhe->bhqk", query, keys, preferred_element_type=jnp.float32
    ) * head_dim ** (-0.5)
    probs = jax.nn.softmax(scores, axis=-1).astype(jnp.bfloat16)
    mixed = jnp.einsum("bhqk,bkhe->bqhe", probs, values, preferred_element_type=jnp.float32).astype(
        jnp.bfloat16
    )
    mixed = mixed.reshape(row_count, quarter)
    attn_part = jnp.dot(
        mixed,
        lax.all_gather(proj_weight, "dp", axis=1, tiled=True),
        preferred_element_type=jnp.float32,
    )
    attn = (
        lax.psum(attn_part.astype(jnp.bfloat16), "mp")
        .astype(jnp.float32)
        .reshape(image_count, tokens, width)
    )
    first_sum = images_f + gate_a[:, None] * attn
    hidden_two = (layer_norm(first_sum) * (1.0 + scale_m[:, None]) + shift_m[:, None]).astype(
        jnp.bfloat16
    )
    hidden_two = hidden_two.reshape(row_count, width)
    ff_quarter = fc1_weight.shape[1]
    columns = hidden_two
    up = jnp.dot(
        columns,
        lax.all_gather(fc1_weight, "dp", axis=0, tiled=True),
        preferred_element_type=jnp.float32,
    )
    gelu_h = (
        jax.nn.gelu(up, approximate=True)
        .astype(jnp.bfloat16)
        .reshape(image_count, tokens, ff_quarter)
    )
    down_full = lax.all_gather(fc2_weight, "dp", axis=1, tiled=True)
    token_share = tokens // lax.axis_size("mp")
    mlp = lax.psum_scatter(
        jnp.einsum("btf,fd->tbd", gelu_h, down_full, preferred_element_type=jnp.float32).astype(
            jnp.bfloat16
        ),
        "mp",
        scatter_dimension=0,
        tiled=True,
    ).astype(jnp.float32)
    token_start = lax.axis_index("mp") * token_share
    own_first = lax.dynamic_slice_in_dim(first_sum, token_start, token_share, 1).transpose(1, 0, 2)
    second_sum = own_first + gate_m[None] * mlp
    fin = (layer_norm(second_sum) * (1.0 + scale_f[None]) + shift_f[None]).astype(jnp.bfloat16)
    noise = jnp.einsum("tbd,do->bto", fin, out_weight, preferred_element_type=jnp.float32)
    noise = noise.reshape(2, pair_count, token_share * out_weight.shape[1])
    noise = lax.all_to_all(noise, "group", split_axis=0, concat_axis=0, tiled=True)
    return noise[1] + guidance[0] * (noise[0] - noise[1])


MESH = pl.DeviceIdType.MESH
BF = jnp.bfloat16
F32 = jnp.float32


def dot_nt(a, b):
    return lax.dot_general(a, b, (((1,), (1,)), ((), ())), preferred_element_type=F32)


class Copies:
    def __init__(self, send, recv):
        self.send, self.recv, self.count, self.sent = send, recv, 0, []

    def slots(self, number):
        first = self.count
        self.count += number
        return first

    def make(self, src, dst, k, dev):
        return pltpu.make_async_remote_copy(
            src_ref=src,
            dst_ref=dst,
            send_sem=self.send.at[k],
            recv_sem=self.recv.at[k],
            device_id=dev,
            device_id_type=MESH,
        )

    def start(self, src, dst, k, dev):
        copy = self.make(src, dst, k, dev)
        copy.start()
        self.sent.append(copy)

    def arrived(self, dst, k, dev):
        self.make(dst, dst, k, dev).wait_recv()

    def drain(self):
        for copy in self.sent:
            copy.wait_send()
        self.sent = []


def copy_count(nd, nm):
    per_weight = 2 * (nd - 1)
    return (
        (nd - 1)
        + (nd * nm - 1)
        + (nm - 1)
        + 3 * per_weight
        + 2 * (nm - 1)
        + per_weight
        + 2 * (nm - 1)
        + (nm - 1)
    )


def block_kernel(
    nd,
    nm,
    head_dim,
    x_ref,
    act_ref,
    ada_ref,
    fada_ref,
    qkv_ref,
    proj_ref,
    fc1_ref,
    fc2_ref,
    outw_ref,
    eps_ref,
    act_all,
    mod_part,
    mod_all,
    fmod_part,
    fmod_all,
    qkv_all,
    proj_all,
    fc1_all,
    fc2_all,
    h_ref,
    q_ref,
    mix_all,
    x1_ref,
    gelu_ref,
    rs_send,
    rs_recv,
    send_sem,
    recv_sem,
):
    g, d, m = lax.axis_index("group"), lax.axis_index("dp"), lax.axis_index("mp")
    images, tokens, width = x_ref.shape
    sib = {"group": 1 - g}

    def dpp(k):
        return lax.rem(d + k + nd, nd)

    def mpp(k):
        return lax.rem(m + k + nm, nm)

    barrier = pltpu.get_barrier_semaphore()
    for a in range(nd):
        for b in range(nm):
            if a or b:
                pl.semaphore_signal(
                    barrier, inc=1, device_id={"dp": dpp(a), "mp": mpp(b)}, device_id_type=MESH
                )
    pl.semaphore_signal(barrier, inc=1, device_id=sib, device_id_type=MESH)
    pl.semaphore_wait(barrier, nd * nm)

    cp = Copies(send_sem, recv_sem)

    k_act = cp.slots(nd - 1)
    for a in range(1, nd):
        cp.start(act_ref, act_all.at[d], k_act + a - 1, {"dp": dpp(a)})
    k_pz = cp.slots(nm - 1)
    for b in range(1, nm):
        cp.start(proj_ref.at[g], proj_all.at[m, d, g], k_pz + b - 1, {"mp": mpp(b)})

    def gather_start(src, buf):
        k = cp.slots(nd - 1)
        for a in range(1, nd):
            cp.start(src.at[g], buf.at[d, g], k + a - 1, {"dp": dpp(a)})
        return k

    def gather_forward(buf, k):
        kf = cp.slots(nd - 1)
        for a in range(1, nd):
            cp.arrived(buf.at[dpp(-a), g], k + a - 1, {"dp": dpp(-a)})
            cp.start(buf.at[dpp(-a), g], buf.at[dpp(-a), g], kf + a - 1, sib)
        return kf

    def gather_finish(buf, kf):
        for a in range(1, nd):
            cp.arrived(buf.at[dpp(-a), 1 - g], kf + a - 1, sib)

    k_qkv = gather_start(qkv_ref, qkv_all)
    act_all[pl.ds(d, 1)] = act_ref[...][None]
    qkv_all[pl.ds(d, 1)] = qkv_ref[...][None]
    proj_all[pl.ds(m, 1), pl.ds(d, 1)] = proj_ref[...][None, None]
    fc1_all[pl.ds(d, 1)] = fc1_ref[...][None]
    fc2_all[pl.ds(d, 1)] = fc2_ref[...][None]

    pad = act_ref.shape[0]
    fpart = jnp.dot(act_ref[...].astype(BF), fada_ref[...], preferred_element_type=F32)
    fmod_part[...] = fpart[:images]
    fmod_all[pl.ds(m, 1)] = fpart[:images][None]
    for a in range(1, nd):
        cp.arrived(act_all.at[dpp(-a)], k_act + a - 1, {"dp": dpp(-a)})
    acts = act_all[...].reshape(nd * pad, act_ref.shape[1]).astype(BF)
    part = jnp.dot(acts, ada_ref[...], preferred_element_type=F32)
    for a in range(nd):
        mod_part[a] = part[a * pad : a * pad + images]
    mod_all[pl.ds(d, 1), pl.ds(m, 1)] = mod_part[pl.ds(d, 1)][None]
    k_mod = cp.slots(nd * nm - 1)
    for a in range(nd):
        for b in range(nm):
            if a or b:
                cp.start(
                    mod_part.at[dpp(a)],
                    mod_all.at[d, m],
                    k_mod + a * nm + b - 1,
                    {"dp": dpp(a), "mp": mpp(b)},
                )
    k_fmod = cp.slots(nm - 1)
    for b in range(1, nm):
        cp.start(fmod_part, fmod_all.at[m], k_fmod + b - 1, {"mp": mpp(b)})

    for b in range(1, nm):
        cp.arrived(proj_all.at[mpp(-b), d, g], k_pz + b - 1, {"mp": mpp(-b)})
    k_pd = cp.slots(nd - 1)
    for a in range(1, nd):
        cp.start(proj_all.at[:, d, g], proj_all.at[:, d, g], k_pd + a - 1, {"dp": dpp(a)})
    k_fc1 = gather_start(fc1_ref, fc1_all)
    k_fc2 = gather_start(fc2_ref, fc2_all)
    f_qkv = gather_forward(qkv_all, k_qkv)
    k_pzs = cp.slots(nm - 1)
    for b in range(1, nm):
        cp.start(
            proj_all.at[mpp(-b), d, g], proj_all.at[mpp(-b), d, g], k_pzs + b - 1, sib
        )

    for a in range(nd):
        for b in range(nm):
            if a or b:
                cp.arrived(
                    mod_all.at[dpp(-a), mpp(-b)],
                    k_mod + a * nm + b - 1,
                    {"dp": dpp(-a), "mp": mpp(-b)},
                )
    mods = jnp.concatenate(
        [functools.reduce(jnp.add, [mod_all[a, b] for b in range(nm)]) for a in range(nd)], axis=1
    )

    def piece(k, i):
        return mods[i : i + 1, k * width : (k + 1) * width]

    step = tokens // 4

    for i in range(images):
        shift, scale = piece(0, i), piece(1, i)

        @pl.loop(0, 4)
        def _(c):
            rows = pl.ds(pl.multiple_of(c * step, step), step)
            v = x_ref[i, rows, :].astype(F32)
            h_ref[i, rows, :] = (layer_norm(v) * (1.0 + scale) + shift).astype(BF)

    gather_finish(qkv_all, f_qkv)
    quarter = qkv_ref.shape[3]
    heads = quarter // head_dim
    lane = lax.broadcasted_iota(jnp.int32, (1, quarter), 1)
    k_mix = cp.slots(images * (nm - 1))
    for i in range(images):
        for j in range(3):
            w = qkv_all[:, :, j].reshape(width, quarter)
            q_ref[j] = jnp.dot(h_ref[i], w, preferred_element_type=F32).astype(BF)
        total = jnp.zeros((tokens, quarter), F32)
        for n in range(heads):
            own = (lane >= n * head_dim) & (lane < (n + 1) * head_dim)
            own = jnp.where(own, 1.0, 0.0).astype(BF)
            s = dot_nt(q_ref[0] * own, q_ref[1]) * head_dim ** (-0.5)
            e = jnp.exp(s - jnp.max(s, axis=-1, keepdims=True))
            p = (e / jnp.sum(e, axis=-1, keepdims=True)).astype(BF)
            total = total + jnp.dot(p, q_ref[2] * own, preferred_element_type=F32)
        mix_all[pl.ds(m, 1), i] = total.astype(BF)[None]
        for b in range(1, nm):
            cp.start(
                mix_all.at[m, i],
                mix_all.at[m, i],
                k_mix + i * (nm - 1) + b - 1,
                {"mp": mpp(b)},
            )

    k_pds = cp.slots(nd - 1)
    for a in range(1, nd):
        cp.arrived(proj_all.at[:, dpp(-a), g], k_pd + a - 1, {"dp": dpp(-a)})
        cp.start(
            proj_all.at[:, dpp(-a), g], proj_all.at[:, dpp(-a), g], k_pds + a - 1, sib
        )
    for b in range(1, nm):
        cp.arrived(proj_all.at[mpp(-b), d, 1 - g], k_pzs + b - 1, sib)
    f_fc1 = gather_forward(fc1_all, k_fc1)
    for a in range(1, nd):
        cp.arrived(proj_all.at[:, dpp(-a), 1 - g], k_pds + a - 1, sib)

    for i in range(images):
        for b in range(1, nm):
            cp.arrived(
                mix_all.at[mpp(-b), i], k_mix + i * (nm - 1) + b - 1, {"mp": mpp(-b)}
            )
        gate, shift, scale = piece(2, i), piece(3, i), piece(4, i)

        @pl.loop(0, 2)
        def _(c):
            rows = pl.ds(pl.multiple_of(c * 2 * step, 2 * step), 2 * step)
            attn = jnp.zeros((2 * step, width), F32)
            for b in range(nm):
                attn = attn + dot_nt(mix_all[b, i, rows, :], proj_all[b].reshape(width, quarter))
            v = x_ref[i, rows, :].astype(F32) + gate * attn
            x1_ref[i, rows, :] = v
            h_ref[i, rows, :] = (layer_norm(v) * (1.0 + scale) + shift).astype(BF)

    gather_finish(fc1_all, f_fc1)
    ff = fc1_ref.shape[2]
    for i in range(images):

        @pl.loop(0, 2)
        def _(c):
            rows = pl.ds(pl.multiple_of(c * 2 * step, 2 * step), 2 * step)
            up = jnp.dot(
                h_ref[i, rows, :], fc1_all[...].reshape(width, ff), preferred_element_type=F32
            )
            gelu_ref[i, rows, :] = jax.nn.gelu(up, approximate=True).astype(BF)

    f_fc2 = gather_forward(fc2_all, k_fc2)
    gather_finish(fc2_all, f_fc2)

    share = tokens // nm
    k_rs = cp.slots(nm - 1)
    own_rows = pl.ds(pl.multiple_of(m * share, share), share)

    def down(rows):
        left = gelu_ref[:, rows, :].reshape(images * share, ff)
        return dot_nt(left, fc2_all[...].reshape(width, ff))

    for b in range(1, nm):
        rows = pl.ds(pl.multiple_of(mpp(b) * share, share), share)
        rs_send[b - 1] = down(rows).astype(BF)
        cp.start(rs_send.at[b - 1], rs_recv.at[b - 1], k_rs + b - 1, {"mp": mpp(b)})
    mlp = down(own_rows)
    for b in range(1, nm):
        cp.arrived(fmod_all.at[mpp(-b)], k_fmod + b - 1, {"mp": mpp(-b)})
    fmods = functools.reduce(jnp.add, [fmod_all[b] for b in range(nm)])
    for b in range(1, nm):
        cp.arrived(rs_recv.at[b - 1], k_rs + b - 1, {"mp": mpp(-b)})
        mlp = mlp + rs_recv[b - 1].astype(F32)
    for i in range(images):
        v = x1_ref[i, own_rows, :] + piece(5, i) * mlp[i * share : (i + 1) * share]
        shift, scale = fmods[i : i + 1, :width], fmods[i : i + 1, width:]
        fin = (layer_norm(v) * (1.0 + scale) + shift).astype(BF)
        eps_ref[i] = jnp.dot(fin, outw_ref[...], preferred_element_type=F32)
    cp.drain()


def on_device_kernel(
    x_arrive,
    cond_first,
    labels,
    step_ids,
    guidance,
    time_table,
    class_table,
    ada_weight,
    final_ada,
    qkv_weight,
    proj_weight,
    fc1_weight,
    fc2_weight,
    out_weight,
):
    nd, nm = lax.axis_size("dp"), lax.axis_size("mp")
    images, tokens, width = x_arrive.shape
    rows, quarter = qkv_weight.shape[1:]
    half = rows // 2
    ff = fc1_weight.shape[1]
    time_part = lax.dynamic_slice_in_dim(time_table, step_ids[0], 1, 0).astype(F32)
    class_part = lax.dynamic_slice_in_dim(class_table, labels[0], 1, 0).astype(F32)
    null_part = class_table[CLASSES].astype(F32)[None, :]
    first = cond_first[0] == 1
    act = jax.nn.silu(
        time_part
        + jnp.concatenate(
            [
                jnp.where(first, class_part, null_part),
                jnp.where(first, null_part, class_part),
            ]
        )
    ).astype(BF)
    act = jnp.pad(act.astype(F32), ((0, 8 - images), (0, 0)))
    qkv_in = qkv_weight.reshape(3, 2, half, quarter).transpose(1, 0, 2, 3)
    proj_in = proj_weight.T.reshape(2, half, quarter)
    fc1_in = fc1_weight.reshape(2, half, ff)
    fc2_in = fc2_weight.T.reshape(2, half, ff)
    copies = copy_count(nd, nm)
    vmem = pl.BlockSpec(memory_space=pltpu.VMEM)
    share = tokens // nm
    eps = pl.pallas_call(
        functools.partial(block_kernel, nd, nm, width // HEADS),
        out_shape=jax.ShapeDtypeStruct((images, share, out_weight.shape[1]), F32),
        in_specs=[vmem] * 9,
        out_specs=vmem,
        scratch_shapes=[
            pltpu.VMEM((nd,) + act.shape, F32),
            pltpu.VMEM((nd, images, ada_weight.shape[1]), F32),
            pltpu.VMEM((nd, nm, images, ada_weight.shape[1]), F32),
            pltpu.VMEM((images, final_ada.shape[1]), F32),
            pltpu.VMEM((nm, images, final_ada.shape[1]), F32),
            pltpu.VMEM((nd, 2, 3, half, quarter), BF),
            pltpu.VMEM((nm, nd, 2, half, quarter), BF),
            pltpu.VMEM((nd, 2, half, ff), BF),
            pltpu.VMEM((nd, 2, half, ff), BF),
            pltpu.VMEM((images, tokens, width), BF),
            pltpu.VMEM((3, tokens, quarter), BF),
            pltpu.VMEM((nm, images, tokens, quarter), BF),
            pltpu.VMEM((images, tokens, width), F32),
            pltpu.VMEM((images, tokens, ff), BF),
            pltpu.VMEM((nm - 1, images * share, width), BF),
            pltpu.VMEM((nm - 1, images * share, width), BF),
            pltpu.SemaphoreType.DMA((copies,)),
            pltpu.SemaphoreType.DMA((copies,)),
        ],
        compiler_params=pltpu.CompilerParams(
            collective_id=0, has_side_effects=True, vmem_limit_bytes=60 * 1024 * 1024
        ),
        name="dit_block",
    )(
        x_arrive,
        act,
        ada_weight,
        final_ada,
        qkv_in,
        proj_in,
        fc1_in,
        fc2_in,
        out_weight,
    )
    cond = jnp.where(first, eps[0], eps[1])
    uncond = jnp.where(first, eps[1], eps[0])
    return (uncond + guidance[0] * (cond - uncond)).reshape(1, share * out_weight.shape[1])


def solution(mesh):
    placed = (
        P(("group", "dp"), None, None),
        P(("group", "dp")),
        P(("group", "dp")),
        P(("group", "dp")),
        P(),
        P(None, "mp"),
        P(None, "mp"),
        P("mp", "dp"),
        P("mp", None),
        P(None, "dp", "mp"),
        P("mp", "dp"),
        P("dp", "mp"),
        P("mp", "dp"),
        P(),
    )
    def body(*args):
        rows = args[9].shape[1]
        fits = args[0].shape[0] == 2 and mesh.shape["group"] == 2 and rows % 32 == 0
        return on_device_kernel(*args) if fits else on_device(*args)

    return jax.shard_map(
        body, mesh=mesh, in_specs=placed, out_specs=P(("group", "dp"), "mp"), check_vma=False
    )
```

```python
import jax
import jax.numpy as jnp
from jax import lax
from jax.experimental import pallas as pl
from jax.experimental.pallas import tpu as pltpu
from jax.sharding import PartitionSpec as P
import functools

HEADS = 16
CLASSES = 1000


def layer_norm(values):
    mean = jnp.mean(values, axis=-1, keepdims=True)
    centred = values - mean
    spread = jnp.mean(centred * centred, axis=-1, keepdims=True)
    return centred * lax.rsqrt(spread + 1e-06)


def on_device(
    x_arrive,
    cond_first,
    labels,
    step_ids,
    guidance,
    time_table,
    class_table,
    ada_weight,
    final_ada,
    qkv_weight,
    proj_weight,
    fc1_weight,
    fc2_weight,
    out_weight,
):
    pair_count = labels.shape[0]
    tokens = x_arrive.shape[1]
    width = x_arrive.shape[2]
    image_count = 2 * pair_count
    row_count = image_count * tokens
    split_rows = x_arrive.reshape(pair_count, 2, tokens, width)
    first = (cond_first == 1)[:, None, None]
    cond_rows = jnp.where(first, split_rows[:, 0], split_rows[:, 1])
    uncond_rows = jnp.where(first, split_rows[:, 1], split_rows[:, 0])
    x_sides = jnp.stack([cond_rows, uncond_rows])
    time_part = jnp.take(time_table, step_ids, axis=0).astype(jnp.float32)
    class_part = jnp.take(class_table, labels, axis=0).astype(jnp.float32)
    null_part = class_table[CLASSES].astype(jnp.float32)[None, :]
    emb_sides = time_part[None] + jnp.stack([class_part, null_part])
    act_sides = jax.nn.silu(emb_sides).astype(jnp.bfloat16)
    images, acts = (
        lax.all_to_all(x_sides, "group", split_axis=0, concat_axis=0, tiled=True),
        lax.all_to_all(act_sides, "group", split_axis=0, concat_axis=0, tiled=True),
    )
    images = images.reshape(image_count, tokens, width)
    acts = acts.reshape(image_count, act_sides.shape[2])
    partial_final = jnp.dot(acts, final_ada, preferred_element_type=jnp.float32)
    every_act = lax.all_gather(acts, "dp", axis=0, tiled=True)
    column_part = jnp.dot(every_act, ada_weight, preferred_element_type=jnp.float32)
    summed, fmods = (
        lax.psum(column_part.astype(jnp.bfloat16), "mp").astype(jnp.float32),
        lax.psum(partial_final.astype(jnp.bfloat16), "mp").astype(jnp.float32),
    )
    mods = lax.all_to_all(
        summed.astype(jnp.bfloat16), "dp", split_axis=0, concat_axis=1, tiled=True
    ).astype(summed.dtype)
    shift_a, scale_a, gate_a, shift_m, scale_m, gate_m = jnp.split(mods, 6, axis=1)
    shift_f, scale_f = jnp.split(fmods, 2, axis=1)
    images_f = images.astype(jnp.float32)
    hidden = (layer_norm(images_f) * (1.0 + scale_a[:, None]) + shift_a[:, None]).astype(
        jnp.bfloat16
    )
    hidden = hidden.reshape(row_count, width)
    quarter = qkv_weight.shape[2]
    head_dim = width // HEADS
    local_heads = quarter // head_dim
    columns = hidden
    qkv = jnp.einsum(
        "rd,kdc->krc",
        columns,
        lax.all_gather(qkv_weight, "dp", axis=1, tiled=True),
        preferred_element_type=jnp.float32,
    ).astype(jnp.bfloat16)
    query = qkv[0].reshape(image_count, tokens, local_heads, head_dim)
    keys = qkv[1].reshape(image_count, tokens, local_heads, head_dim)
    values = qkv[2].reshape(image_count, tokens, local_heads, head_dim)
    scores = jnp.einsum(
        "bqhe,bkhe->bhqk", query, keys, preferred_element_type=jnp.float32
    ) * head_dim ** (-0.5)
    probs = jax.nn.softmax(scores, axis=-1).astype(jnp.bfloat16)
    mixed = jnp.einsum("bhqk,bkhe->bqhe", probs, values, preferred_element_type=jnp.float32).astype(
        jnp.bfloat16
    )
    mixed = mixed.reshape(row_count, quarter)
    attn_part = jnp.dot(
        mixed,
        lax.all_gather(proj_weight, "dp", axis=1, tiled=True),
        preferred_element_type=jnp.float32,
    )
    attn = (
        lax.psum(attn_part.astype(jnp.bfloat16), "mp")
        .astype(jnp.float32)
        .reshape(image_count, tokens, width)
    )
    first_sum = images_f + gate_a[:, None] * attn
    hidden_two = (layer_norm(first_sum) * (1.0 + scale_m[:, None]) + shift_m[:, None]).astype(
        jnp.bfloat16
    )
    hidden_two = hidden_two.reshape(row_count, width)
    ff_quarter = fc1_weight.shape[1]
    columns = hidden_two
    up = jnp.dot(
        columns,
        lax.all_gather(fc1_weight, "dp", axis=0, tiled=True),
        preferred_element_type=jnp.float32,
    )
    gelu_h = (
        jax.nn.gelu(up, approximate=True)
        .astype(jnp.bfloat16)
        .reshape(image_count, tokens, ff_quarter)
    )
    down_full = lax.all_gather(fc2_weight, "dp", axis=1, tiled=True)
    token_share = tokens // lax.axis_size("mp")
    mlp = lax.psum_scatter(
        jnp.einsum("btf,fd->tbd", gelu_h, down_full, preferred_element_type=jnp.float32).astype(
            jnp.bfloat16
        ),
        "mp",
        scatter_dimension=0,
        tiled=True,
    ).astype(jnp.float32)
    token_start = lax.axis_index("mp") * token_share
    own_first = lax.dynamic_slice_in_dim(first_sum, token_start, token_share, 1).transpose(1, 0, 2)
    second_sum = own_first + gate_m[None] * mlp
    fin = (layer_norm(second_sum) * (1.0 + scale_f[None]) + shift_f[None]).astype(jnp.bfloat16)
    noise = jnp.einsum("tbd,do->bto", fin, out_weight, preferred_element_type=jnp.float32)
    noise = noise.reshape(2, pair_count, token_share * out_weight.shape[1])
    noise = lax.all_to_all(noise, "group", split_axis=0, concat_axis=0, tiled=True)
    return noise[1] + guidance[0] * (noise[0] - noise[1])


MESH = pl.DeviceIdType.MESH
BF = jnp.bfloat16
F32 = jnp.float32


def dot_nt(a, b):
    return lax.dot_general(a, b, (((1,), (1,)), ((), ())), preferred_element_type=F32)


class Copies:
    def __init__(self, send, recv):
        self.send, self.recv, self.count, self.sent = send, recv, 0, []

    def slots(self, number):
        first = self.count
        self.count += number
        return first

    def make(self, src, dst, k, dev):
        return pltpu.make_async_remote_copy(
            src_ref=src,
            dst_ref=dst,
            send_sem=self.send.at[k],
            recv_sem=self.recv.at[k],
            device_id=dev,
            device_id_type=MESH,
        )

    def start(self, src, dst, k, dev):
        copy = self.make(src, dst, k, dev)
        copy.start()
        self.sent.append(copy)

    def arrived(self, dst, k, dev):
        self.make(dst, dst, k, dev).wait_recv()

    def drain(self):
        for copy in self.sent:
            copy.wait_send()
        self.sent = []


def copy_count(nd, nm):
    gather = 2 + 2 + nd
    return (
        (nd - 1) + (nm - 1) + (nd * nm - 1) + (nm - 1) + 4 * gather + 4 * (nm - 1) + 2 * (nm - 1)
    )


def block_kernel(
    nd,
    nm,
    head_dim,
    x_ref,
    act_ref,
    ada_ref,
    fada_ref,
    qkv_ref,
    proj_ref,
    fc1_ref,
    fc2_ref,
    outw_ref,
    eps_ref,
    act_all,
    mod_part,
    mod_all,
    fmod_part,
    fmod_all,
    qkv_all,
    proj_z,
    proj_all,
    fc1_all,
    fc2_all,
    h_ref,
    mix_all,
    x1_ref,
    gelu_ref,
    rs_send,
    rs_recv,
    send_sem,
    recv_sem,
):
    g, d, m = lax.axis_index("group"), lax.axis_index("dp"), lax.axis_index("mp")
    images, tokens, width = x_ref.shape
    half = fc1_ref.shape[1]
    low = (half + 31) // 32 * 16
    parts = (pl.ds(0, low), pl.ds(low, half - low))
    sib = {"group": 1 - g}
    near = (d + 1 - 2 * lax.rem(d, 2), lax.rem(d + 2, nd))
    diag = nd - 1 - d

    def dpp(k):
        return lax.rem(d + k + nd, nd)

    def mpp(k):
        return lax.rem(m + k + nm, nm)

    barrier = pltpu.get_barrier_semaphore()
    for a in range(nd):
        for b in range(nm):
            if a or b:
                pl.semaphore_signal(
                    barrier, inc=1, device_id={"dp": dpp(a), "mp": mpp(b)}, device_id_type=MESH
                )
    pl.semaphore_signal(barrier, inc=1, device_id=sib, device_id_type=MESH)
    pl.semaphore_wait(barrier, nd * nm)

    cp = Copies(send_sem, recv_sem)

    class Gather:
        def __init__(self, buf, own_too=False):
            self.buf, self.k, self.own_too = buf, cp.slots(2 + 2 + nd), own_too

        def begin(self, src):
            for n in range(2):
                cp.start(src, self.buf.at[d, g], self.k + n, {"dp": near[n]})

        def share(self, slot, n):
            cp.start(self.buf.at[slot, g], self.buf.at[slot, g], self.k + 4 + n, sib)

        def relay(self):
            if self.own_too:
                self.share(d, 0)
            for n in range(2):
                cp.arrived(self.buf.at[near[n], g], self.k + n, {"dp": near[n]})
                piece = self.buf.at[near[n], g, parts[n]]
                cp.start(piece, piece, self.k + 2 + n, {"dp": near[1 - n]})
                self.share(near[n], 1 + n)

        def last(self):
            for n in range(2):
                piece = self.buf.at[diag, g, parts[n]]
                cp.arrived(piece, self.k + 2 + n, {"dp": near[1 - n]})
            self.share(diag, 3)

        def finish(self):
            if self.own_too:
                cp.arrived(self.buf.at[d, 1 - g], self.k + 4, sib)
            for n, slot in enumerate((near[0], near[1], diag)):
                cp.arrived(self.buf.at[slot, 1 - g], self.k + 5 + n, sib)

    k_act = cp.slots(nd - 1)
    for a in range(1, nd):
        cp.start(act_ref, act_all.at[d], k_act + a - 1, {"dp": dpp(a)})
    qkv = Gather(qkv_all)
    qkv.begin(qkv_ref.at[g])
    k_pz = cp.slots(nm - 1)
    for b in range(1, nm):
        cp.start(proj_ref.at[g], proj_z.at[m], k_pz + b - 1, {"mp": mpp(b)})

    act_all[pl.ds(d, 1)] = act_ref[...][None]
    qkv_all[pl.ds(d, 1)] = qkv_ref[...][None]
    proj_z[pl.ds(m, 1)] = proj_ref[pl.ds(g, 1)]
    fc1_all[pl.ds(d, 1)] = fc1_ref[...][None]
    fc2_all[pl.ds(d, 1)] = fc2_ref[...][None]

    pad = act_ref.shape[0]
    fpart = jnp.dot(act_ref[...].astype(BF), fada_ref[...], preferred_element_type=F32)
    fmod_part[...] = fpart[:images]
    fmod_all[pl.ds(m, 1)] = fpart[:images][None]
    for a in range(1, nd):
        cp.arrived(act_all.at[dpp(-a)], k_act + a - 1, {"dp": dpp(-a)})
    acts = act_all[...].reshape(nd * pad, act_ref.shape[1]).astype(BF)
    part = jnp.dot(acts, ada_ref[...], preferred_element_type=F32)
    for a in range(nd):
        mod_part[a] = part[a * pad : a * pad + images]
    mod_all[pl.ds(d, 1), pl.ds(m, 1)] = mod_part[pl.ds(d, 1)][None]
    k_mod = cp.slots(nd * nm - 1)
    for a in range(nd):
        for b in range(nm):
            if a or b:
                cp.start(
                    mod_part.at[dpp(a)],
                    mod_all.at[d, m],
                    k_mod + a * nm + b - 1,
                    {"dp": dpp(a), "mp": mpp(b)},
                )
    k_fmod = cp.slots(nm - 1)
    for b in range(1, nm):
        cp.start(fmod_part, fmod_all.at[m], k_fmod + b - 1, {"mp": mpp(b)})

    qkv.relay()
    fc1 = Gather(fc1_all)
    fc1.begin(fc1_ref.at[g])

    for b in range(1, nm):
        cp.arrived(proj_z.at[mpp(-b)], k_pz + b - 1, {"mp": mpp(-b)})
    proj_all[pl.ds(d, 1), pl.ds(g, 1)] = jnp.concatenate(
        [proj_z[b] for b in range(nm)], axis=1
    )[None, None]
    for a in range(nd):
        for b in range(nm):
            if a or b:
                cp.arrived(
                    mod_all.at[dpp(-a), mpp(-b)],
                    k_mod + a * nm + b - 1,
                    {"dp": dpp(-a), "mp": mpp(-b)},
                )
    mods = jnp.concatenate(
        [functools.reduce(jnp.add, [mod_all[a, b] for b in range(nm)]) for a in range(nd)], axis=1
    )

    def piece(k, i):
        return mods[i : i + 1, k * width : (k + 1) * width]

    step = tokens // 4

    for i in range(images):
        shift, scale = piece(0, i), piece(1, i)

        @pl.loop(0, 4)
        def _(c):
            rows = pl.ds(pl.multiple_of(c * step, step), step)
            v = x_ref[i, rows, :].astype(F32)
            h_ref[i, rows, :] = (layer_norm(v) * (1.0 + scale) + shift).astype(BF)

    qkv.last()
    proj = Gather(proj_all, own_too=True)
    proj.begin(proj_all.at[d, g])
    qkv.finish()

    quarter = qkv_ref.shape[2] // 3
    heads = quarter // head_dim
    lane = lax.broadcasted_iota(jnp.int32, (1, quarter), 1)
    k_mix = cp.slots(4 * (nm - 1))
    fc2 = Gather(fc2_all)
    held = []

    def hop(i, h):
        for way, sign in ((0, 1), (1, -1)):
            k = k_mix + (way * 2 + i) * (nm - 1)
            origin = m - sign * h
            there = (m >= h) if way == 0 else (m < nm - h)
            room = (m < nm - 1) if way == 0 else (m > 0)
            block = mix_all.at[jnp.clip(origin, 0, nm - 1), i]
            if h:

                @pl.when(there)
                def _():
                    cp.make(block, block, k + h - 1, {"mp": mpp(-sign)}).wait_recv()

            if h < nm - 1:
                copy = cp.make(block, block, k + h, {"mp": mpp(sign)})
                held.append((there & room, copy))

                @pl.when(there & room)
                def _():
                    copy.start()

    for i in range(images):
        w = qkv_all[...].reshape(width, 3 * quarter)
        mixed3 = jnp.dot(h_ref[i], w, preferred_element_type=F32).astype(BF)
        query, key, value = (mixed3[:, j * quarter : (j + 1) * quarter] for j in range(3))
        total = jnp.zeros((tokens, quarter), F32)
        for n in range(heads):
            own = (lane >= n * head_dim) & (lane < (n + 1) * head_dim)
            own = jnp.where(own, 1.0, 0.0).astype(BF)
            s = dot_nt(query * own, key) * head_dim ** (-0.5)
            e = jnp.exp(s - jnp.max(s, axis=-1, keepdims=True))
            p = (e / jnp.sum(e, axis=-1, keepdims=True)).astype(BF)
            total = total + jnp.dot(p, value * own, preferred_element_type=F32)
        mix_all[pl.ds(m, 1), i] = total.T.astype(BF)[None]
        hop(i, 0)
        if i == 0:
            fc1.relay()
            fc2.begin(fc2_ref.at[g])

    hop(0, 1)
    proj.relay()
    hop(1, 1)
    fc1.last()
    hop(0, 2)
    hop(1, 2)
    proj.last()
    fc2.relay()
    hop(0, 3)
    proj.finish()

    ff = fc1_ref.shape[2]
    share = tokens // nm
    k_rs = cp.slots(2 * (nm - 1))
    for i in range(images):
        if i:
            hop(i, 3)
        gate, shift, scale = piece(2, i), piece(3, i), piece(4, i)
        full = mix_all[:, i].reshape(width, tokens).T
        attn = dot_nt(full, proj_all[...].reshape(width, width))
        x1_ref[i] = attn

        @pl.loop(0, 4)
        def _(c):
            rows = pl.ds(pl.multiple_of(c * step, step), step)
            v = x_ref[i, rows, :].astype(F32) + gate * x1_ref[i, rows, :]
            x1_ref[i, rows, :] = v
            h_ref[i, rows, :] = (layer_norm(v) * (1.0 + scale) + shift).astype(BF)

        if i == 0:
            fc1.finish()

        @pl.loop(0, 2)
        def _(c):
            rows = pl.ds(pl.multiple_of(c * 2 * step, 2 * step), 2 * step)
            up = jnp.dot(
                h_ref[i, rows, :], fc1_all[...].reshape(width, ff), preferred_element_type=F32
            )
            gelu_ref[i, rows, :] = jax.nn.gelu(up, approximate=True).astype(BF)

        if i == 0:
            fc2.last()
            fc2.finish()
        rs_send[i] = dot_nt(gelu_ref[i], fc2_all[...].reshape(width, ff)).astype(BF)
        for b in range(1, nm):
            rows = pl.ds(pl.multiple_of(mpp(b) * share, share), share)
            cp.start(
                rs_send.at[i, rows],
                rs_recv.at[i, b - 1],
                k_rs + i * (nm - 1) + b - 1,
                {"mp": mpp(b)},
            )

    own_rows = pl.ds(pl.multiple_of(m * share, share), share)
    for b in range(1, nm):
        cp.arrived(fmod_all.at[mpp(-b)], k_fmod + b - 1, {"mp": mpp(-b)})
    fmods = functools.reduce(jnp.add, [fmod_all[b] for b in range(nm)])
    for i in range(images):
        mlp = rs_send[i, own_rows, :].astype(F32)
        for b in range(1, nm):
            cp.arrived(rs_recv.at[i, b - 1], k_rs + i * (nm - 1) + b - 1, {"mp": mpp(-b)})
            mlp = mlp + rs_recv[i, b - 1].astype(F32)
        v = x1_ref[i, own_rows, :] + piece(5, i) * mlp
        shift, scale = fmods[i : i + 1, :width], fmods[i : i + 1, width:]
        fin = (layer_norm(v) * (1.0 + scale) + shift).astype(BF)
        eps_ref[i] = jnp.dot(fin, outw_ref[...], preferred_element_type=F32)
    cp.drain()
    for cond, copy in held:

        @pl.when(cond)
        def _():
            copy.wait_send()


def on_device_kernel(
    x_arrive,
    cond_first,
    labels,
    step_ids,
    guidance,
    time_table,
    class_table,
    ada_weight,
    final_ada,
    qkv_weight,
    proj_weight,
    fc1_weight,
    fc2_weight,
    out_weight,
):
    nd, nm = lax.axis_size("dp"), lax.axis_size("mp")
    images, tokens, width = x_arrive.shape
    rows, quarter = qkv_weight.shape[1:]
    half = rows // 2
    ff = fc1_weight.shape[1]
    time_part = lax.dynamic_slice_in_dim(time_table, step_ids[0], 1, 0).astype(F32)
    class_part = lax.dynamic_slice_in_dim(class_table, labels[0], 1, 0).astype(F32)
    null_part = class_table[CLASSES].astype(F32)[None, :]
    first = cond_first[0] == 1
    act = jax.nn.silu(
        time_part
        + jnp.concatenate(
            [
                jnp.where(first, class_part, null_part),
                jnp.where(first, null_part, class_part),
            ]
        )
    ).astype(BF)
    act = jnp.pad(act.astype(F32), ((0, 8 - images), (0, 0)))
    qkv_in = qkv_weight.transpose(1, 0, 2).reshape(2, half, 3 * quarter)
    proj_in = proj_weight.T.reshape(2, half, quarter)
    fc1_in = fc1_weight.reshape(2, half, ff)
    fc2_in = fc2_weight.T.reshape(2, half, ff)
    copies = copy_count(nd, nm)
    vmem = pl.BlockSpec(memory_space=pltpu.VMEM)
    share = tokens // nm
    eps = pl.pallas_call(
        functools.partial(block_kernel, nd, nm, width // HEADS),
        out_shape=jax.ShapeDtypeStruct((images, share, out_weight.shape[1]), F32),
        in_specs=[vmem] * 9,
        out_specs=vmem,
        scratch_shapes=[
            pltpu.VMEM((nd,) + act.shape, F32),
            pltpu.VMEM((nd, images, ada_weight.shape[1]), F32),
            pltpu.VMEM((nd, nm, images, ada_weight.shape[1]), F32),
            pltpu.VMEM((images, final_ada.shape[1]), F32),
            pltpu.VMEM((nm, images, final_ada.shape[1]), F32),
            pltpu.VMEM((nd, 2, half, 3 * quarter), BF),
            pltpu.VMEM((nm, half, quarter), BF),
            pltpu.VMEM((nd, 2, half, width), BF),
            pltpu.VMEM((nd, 2, half, ff), BF),
            pltpu.VMEM((nd, 2, half, ff), BF),
            pltpu.VMEM((images, tokens, width), BF),
            pltpu.VMEM((nm, images, quarter, tokens), BF),
            pltpu.VMEM((images, tokens, width), F32),
            pltpu.VMEM((images, tokens, ff), BF),
            pltpu.VMEM((images, tokens, width), BF),
            pltpu.VMEM((images, nm - 1, share, width), BF),
            pltpu.SemaphoreType.DMA((copies,)),
            pltpu.SemaphoreType.DMA((copies,)),
        ],
        compiler_params=pltpu.CompilerParams(
            collective_id=0, has_side_effects=True, vmem_limit_bytes=60 * 1024 * 1024
        ),
        name="dit_block",
    )(
        x_arrive,
        act,
        ada_weight,
        final_ada,
        qkv_in,
        proj_in,
        fc1_in,
        fc2_in,
        out_weight,
    )
    cond = jnp.where(first, eps[0], eps[1])
    uncond = jnp.where(first, eps[1], eps[0])
    return (uncond + guidance[0] * (cond - uncond)).reshape(1, share * out_weight.shape[1])


def solution(mesh):
    placed = (
        P(("group", "dp"), None, None),
        P(("group", "dp")),
        P(("group", "dp")),
        P(("group", "dp")),
        P(),
        P(None, "mp"),
        P(None, "mp"),
        P("mp", "dp"),
        P("mp", None),
        P(None, "dp", "mp"),
        P("mp", "dp"),
        P("dp", "mp"),
        P("mp", "dp"),
        P(),
    )
    def body(*args):
        rows = args[9].shape[1]
        fits = args[0].shape[0] == 2 and mesh.shape["group"] == 2 and rows % 32 == 0
        fits = fits and mesh.shape["dp"] == 4 and mesh.shape["mp"] == 4
        return on_device_kernel(*args) if fits else on_device(*args)

    return jax.shard_map(
        body, mesh=mesh, in_specs=placed, out_specs=P(("group", "dp"), "mp"), check_vma=False
    )
```

```python
import jax
import jax.numpy as jnp
from jax import lax
from jax.experimental import pallas as pl
from jax.experimental.pallas import tpu as pltpu
from jax.sharding import PartitionSpec as P
import functools

HEADS = 16
CLASSES = 1000


def layer_norm(values):
    mean = jnp.mean(values, axis=-1, keepdims=True)
    centred = values - mean
    spread = jnp.mean(centred * centred, axis=-1, keepdims=True)
    return centred * lax.rsqrt(spread + 1e-06)


def on_device(
    x_arrive,
    cond_first,
    labels,
    step_ids,
    guidance,
    time_table,
    class_table,
    ada_weight,
    final_ada,
    qkv_weight,
    proj_weight,
    fc1_weight,
    fc2_weight,
    out_weight,
):
    pair_count = labels.shape[0]
    tokens = x_arrive.shape[1]
    width = x_arrive.shape[2]
    image_count = 2 * pair_count
    row_count = image_count * tokens
    split_rows = x_arrive.reshape(pair_count, 2, tokens, width)
    first = (cond_first == 1)[:, None, None]
    cond_rows = jnp.where(first, split_rows[:, 0], split_rows[:, 1])
    uncond_rows = jnp.where(first, split_rows[:, 1], split_rows[:, 0])
    x_sides = jnp.stack([cond_rows, uncond_rows])
    time_part = jnp.take(time_table, step_ids, axis=0).astype(jnp.float32)
    class_part = jnp.take(class_table, labels, axis=0).astype(jnp.float32)
    null_part = class_table[CLASSES].astype(jnp.float32)[None, :]
    emb_sides = time_part[None] + jnp.stack([class_part, null_part])
    act_sides = jax.nn.silu(emb_sides).astype(jnp.bfloat16)
    images, acts = (
        lax.all_to_all(x_sides, "group", split_axis=0, concat_axis=0, tiled=True),
        lax.all_to_all(act_sides, "group", split_axis=0, concat_axis=0, tiled=True),
    )
    images = images.reshape(image_count, tokens, width)
    acts = acts.reshape(image_count, act_sides.shape[2])
    partial_final = jnp.dot(acts, final_ada, preferred_element_type=jnp.float32)
    every_act = lax.all_gather(acts, "dp", axis=0, tiled=True)
    column_part = jnp.dot(every_act, ada_weight, preferred_element_type=jnp.float32)
    summed, fmods = (
        lax.psum(column_part.astype(jnp.bfloat16), "mp").astype(jnp.float32),
        lax.psum(partial_final.astype(jnp.bfloat16), "mp").astype(jnp.float32),
    )
    mods = lax.all_to_all(
        summed.astype(jnp.bfloat16), "dp", split_axis=0, concat_axis=1, tiled=True
    ).astype(summed.dtype)
    shift_a, scale_a, gate_a, shift_m, scale_m, gate_m = jnp.split(mods, 6, axis=1)
    shift_f, scale_f = jnp.split(fmods, 2, axis=1)
    images_f = images.astype(jnp.float32)
    hidden = (layer_norm(images_f) * (1.0 + scale_a[:, None]) + shift_a[:, None]).astype(
        jnp.bfloat16
    )
    hidden = hidden.reshape(row_count, width)
    quarter = qkv_weight.shape[2]
    head_dim = width // HEADS
    local_heads = quarter // head_dim
    columns = hidden
    qkv = jnp.einsum(
        "rd,kdc->krc",
        columns,
        lax.all_gather(qkv_weight, "dp", axis=1, tiled=True),
        preferred_element_type=jnp.float32,
    ).astype(jnp.bfloat16)
    query = qkv[0].reshape(image_count, tokens, local_heads, head_dim)
    keys = qkv[1].reshape(image_count, tokens, local_heads, head_dim)
    values = qkv[2].reshape(image_count, tokens, local_heads, head_dim)
    scores = jnp.einsum(
        "bqhe,bkhe->bhqk", query, keys, preferred_element_type=jnp.float32
    ) * head_dim ** (-0.5)
    probs = jax.nn.softmax(scores, axis=-1).astype(jnp.bfloat16)
    mixed = jnp.einsum("bhqk,bkhe->bqhe", probs, values, preferred_element_type=jnp.float32).astype(
        jnp.bfloat16
    )
    mixed = mixed.reshape(row_count, quarter)
    attn_part = jnp.dot(
        mixed,
        lax.all_gather(proj_weight, "dp", axis=1, tiled=True),
        preferred_element_type=jnp.float32,
    )
    attn = (
        lax.psum(attn_part.astype(jnp.bfloat16), "mp")
        .astype(jnp.float32)
        .reshape(image_count, tokens, width)
    )
    first_sum = images_f + gate_a[:, None] * attn
    hidden_two = (layer_norm(first_sum) * (1.0 + scale_m[:, None]) + shift_m[:, None]).astype(
        jnp.bfloat16
    )
    hidden_two = hidden_two.reshape(row_count, width)
    ff_quarter = fc1_weight.shape[1]
    columns = hidden_two
    up = jnp.dot(
        columns,
        lax.all_gather(fc1_weight, "dp", axis=0, tiled=True),
        preferred_element_type=jnp.float32,
    )
    gelu_h = (
        jax.nn.gelu(up, approximate=True)
        .astype(jnp.bfloat16)
        .reshape(image_count, tokens, ff_quarter)
    )
    down_full = lax.all_gather(fc2_weight, "dp", axis=1, tiled=True)
    token_share = tokens // lax.axis_size("mp")
    mlp = lax.psum_scatter(
        jnp.einsum("btf,fd->tbd", gelu_h, down_full, preferred_element_type=jnp.float32).astype(
            jnp.bfloat16
        ),
        "mp",
        scatter_dimension=0,
        tiled=True,
    ).astype(jnp.float32)
    token_start = lax.axis_index("mp") * token_share
    own_first = lax.dynamic_slice_in_dim(first_sum, token_start, token_share, 1).transpose(1, 0, 2)
    second_sum = own_first + gate_m[None] * mlp
    fin = (layer_norm(second_sum) * (1.0 + scale_f[None]) + shift_f[None]).astype(jnp.bfloat16)
    noise = jnp.einsum("tbd,do->bto", fin, out_weight, preferred_element_type=jnp.float32)
    noise = noise.reshape(2, pair_count, token_share * out_weight.shape[1])
    noise = lax.all_to_all(noise, "group", split_axis=0, concat_axis=0, tiled=True)
    return noise[1] + guidance[0] * (noise[0] - noise[1])


MESH = pl.DeviceIdType.MESH
BF = jnp.bfloat16
F32 = jnp.float32


def dot_nt(a, b):
    return lax.dot_general(a, b, (((1,), (1,)), ((), ())), preferred_element_type=F32)


class Copies:
    def __init__(self, send, recv):
        self.send, self.recv, self.count, self.sent = send, recv, 0, []

    def slots(self, number):
        first = self.count
        self.count += number
        return first

    def make(self, src, dst, k, dev):
        return pltpu.make_async_remote_copy(
            src_ref=src,
            dst_ref=dst,
            send_sem=self.send.at[k],
            recv_sem=self.recv.at[k],
            device_id=dev,
            device_id_type=MESH,
        )

    def start(self, src, dst, k, dev):
        copy = self.make(src, dst, k, dev)
        copy.start()
        self.sent.append(copy)

    def arrived(self, dst, k, dev):
        self.make(dst, dst, k, dev).wait_recv()

    def drain(self):
        for copy in self.sent:
            copy.wait_send()
        self.sent = []


def copy_count(nd, nm):
    gather = 2 + 2 + nd
    return (
        (nd - 1) + (nm - 1) + (nd * nm - 1) + (nm - 1) + 4 * gather + 4 * (nm - 1) + 2 * (nm - 1)
    )


def block_kernel(
    nd,
    nm,
    head_dim,
    x_ref,
    act_ref,
    ada_ref,
    fada_ref,
    qkv_ref,
    proj_ref,
    fc1_ref,
    fc2_ref,
    outw_ref,
    eps_ref,
    act_all,
    mod_part,
    mod_all,
    fmod_part,
    fmod_all,
    qkv_all,
    proj_own,
    proj_z,
    proj_all,
    fc1_all,
    fc2_all,
    h_ref,
    mix_all,
    x1_ref,
    gelu_ref,
    rs_send,
    rs_recv,
    send_sem,
    recv_sem,
):
    g, d, m = lax.axis_index("group"), lax.axis_index("dp"), lax.axis_index("mp")
    images, tokens, width = x_ref.shape
    half = fc1_ref.shape[1]
    low = (half + 31) // 32 * 16
    parts = (pl.ds(0, low), pl.ds(low, half - low))
    sib = {"group": 1 - g}
    near = (d + 1 - 2 * lax.rem(d, 2), lax.rem(d + 2, nd))
    diag = nd - 1 - d

    def dpp(k):
        return lax.rem(d + k + nd, nd)

    def mpp(k):
        return lax.rem(m + k + nm, nm)

    quarter = qkv_ref.shape[2]
    for n in range(2):
        cut = slice(n * half, (n + 1) * half)
        qkv_all[pl.ds(d, 1), n] = jnp.concatenate(
            [qkv_ref[j, cut, :] for j in range(3)], axis=1
        )[None]
    proj_own[...] = proj_ref[...].astype(F32).T.astype(BF).reshape(proj_own.shape)

    barrier = pltpu.get_barrier_semaphore()
    for a in range(nd):
        for b in range(nm):
            if a or b:
                pl.semaphore_signal(
                    barrier, inc=1, device_id={"dp": dpp(a), "mp": mpp(b)}, device_id_type=MESH
                )
    pl.semaphore_signal(barrier, inc=1, device_id=sib, device_id_type=MESH)
    pl.semaphore_wait(barrier, nd * nm)

    cp = Copies(send_sem, recv_sem)

    class Gather:
        def __init__(self, buf, own_too=False):
            self.buf, self.k, self.own_too = buf, cp.slots(2 + 2 + nd), own_too

        def begin(self, src):
            for n in range(2):
                cp.start(src, self.buf.at[d, g], self.k + n, {"dp": near[n]})

        def share(self, slot, n):
            cp.start(self.buf.at[slot, g], self.buf.at[slot, g], self.k + 4 + n, sib)

        def relay(self):
            if self.own_too:
                self.share(d, 0)
            for n in range(2):
                cp.arrived(self.buf.at[near[n], g], self.k + n, {"dp": near[n]})
                piece = self.buf.at[near[n], g, parts[n]]
                cp.start(piece, piece, self.k + 2 + n, {"dp": near[1 - n]})
                self.share(near[n], 1 + n)

        def last(self):
            for n in range(2):
                piece = self.buf.at[diag, g, parts[n]]
                cp.arrived(piece, self.k + 2 + n, {"dp": near[1 - n]})
            self.share(diag, 3)

        def finish(self):
            if self.own_too:
                cp.arrived(self.buf.at[d, 1 - g], self.k + 4, sib)
            for n, slot in enumerate((near[0], near[1], diag)):
                cp.arrived(self.buf.at[slot, 1 - g], self.k + 5 + n, sib)

    k_act = cp.slots(nd - 1)
    for a in range(1, nd):
        cp.start(act_ref, act_all.at[d], k_act + a - 1, {"dp": dpp(a)})
    qkv = Gather(qkv_all)
    qkv.begin(qkv_all.at[d, g])
    k_pz = cp.slots(nm - 1)
    for b in range(1, nm):
        cp.start(proj_own.at[g], proj_z.at[m], k_pz + b - 1, {"mp": mpp(b)})

    act_all[pl.ds(d, 1)] = act_ref[...][None]
    proj_z[pl.ds(m, 1)] = proj_own[pl.ds(g, 1)]
    fc1_all[pl.ds(d, 1)] = fc1_ref[...][None]
    fc2_all[pl.ds(d, 1)] = fc2_ref[...][None]

    pad = act_ref.shape[0]
    fpart = jnp.dot(act_ref[...].astype(BF), fada_ref[...], preferred_element_type=F32)
    fmod_part[...] = fpart[:images]
    fmod_all[pl.ds(m, 1)] = fpart[:images][None]
    for a in range(1, nd):
        cp.arrived(act_all.at[dpp(-a)], k_act + a - 1, {"dp": dpp(-a)})
    acts = act_all[...].reshape(nd * pad, act_ref.shape[1]).astype(BF)
    part = jnp.dot(acts, ada_ref[...], preferred_element_type=F32)
    for a in range(nd):
        mod_part[a] = part[a * pad : a * pad + images]
    mod_all[pl.ds(d, 1), pl.ds(m, 1)] = mod_part[pl.ds(d, 1)][None]
    k_mod = cp.slots(nd * nm - 1)
    for a in range(nd):
        for b in range(nm):
            if a or b:
                cp.start(
                    mod_part.at[dpp(a)],
                    mod_all.at[d, m],
                    k_mod + a * nm + b - 1,
                    {"dp": dpp(a), "mp": mpp(b)},
                )
    k_fmod = cp.slots(nm - 1)
    for b in range(1, nm):
        cp.start(fmod_part, fmod_all.at[m], k_fmod + b - 1, {"mp": mpp(b)})

    qkv.relay()
    fc1 = Gather(fc1_all)
    fc1.begin(fc1_ref.at[g])

    for a in range(nd):
        for b in range(nm):
            if a or b:
                cp.arrived(
                    mod_all.at[dpp(-a), mpp(-b)],
                    k_mod + a * nm + b - 1,
                    {"dp": dpp(-a), "mp": mpp(-b)},
                )
    mods = jnp.concatenate(
        [functools.reduce(jnp.add, [mod_all[a, b] for b in range(nm)]) for a in range(nd)], axis=1
    )

    def piece(k, i):
        return mods[i : i + 1, k * width : (k + 1) * width]

    step = tokens // 4

    for i in range(images):
        shift, scale = piece(0, i), piece(1, i)

        @pl.loop(0, 4)
        def _(c):
            rows = pl.ds(pl.multiple_of(c * step, step), step)
            v = x_ref[i, rows, :].astype(F32)
            h_ref[i, rows, :] = (layer_norm(v) * (1.0 + scale) + shift).astype(BF)

    qkv.last()
    for b in range(1, nm):
        cp.arrived(proj_z.at[mpp(-b)], k_pz + b - 1, {"mp": mpp(-b)})
    proj_all[pl.ds(d, 1), pl.ds(g, 1)] = jnp.concatenate(
        [proj_z[b] for b in range(nm)], axis=1
    )[None, None]
    proj = Gather(proj_all, own_too=True)
    proj.begin(proj_all.at[d, g])
    qkv.finish()

    heads = quarter // head_dim
    lane = lax.broadcasted_iota(jnp.int32, (1, quarter), 1)
    k_mix = cp.slots(4 * (nm - 1))
    fc2 = Gather(fc2_all)
    held = []

    def hop(i, h):
        for way, sign in ((0, 1), (1, -1)):
            k = k_mix + (way * 2 + i) * (nm - 1)
            origin = m - sign * h
            there = (m >= h) if way == 0 else (m < nm - h)
            room = (m < nm - 1) if way == 0 else (m > 0)
            block = mix_all.at[jnp.clip(origin, 0, nm - 1), i]
            if h:

                @pl.when(there)
                def _():
                    cp.make(block, block, k + h - 1, {"mp": mpp(-sign)}).wait_recv()

            if h < nm - 1:
                copy = cp.make(block, block, k + h, {"mp": mpp(sign)})
                held.append((there & room, copy))

                @pl.when(there & room)
                def _():
                    copy.start()

    for i in range(images):
        w = qkv_all[...].reshape(width, 3 * quarter)
        mixed3 = jnp.dot(h_ref[i], w, preferred_element_type=F32).astype(BF)
        query, key, value = (mixed3[:, j * quarter : (j + 1) * quarter] for j in range(3))
        total = jnp.zeros((tokens, quarter), F32)
        for n in range(heads):
            own = (lane >= n * head_dim) & (lane < (n + 1) * head_dim)
            own = jnp.where(own, 1.0, 0.0).astype(BF)
            s = dot_nt(query * own, key) * head_dim ** (-0.5)
            e = jnp.exp(s - jnp.max(s, axis=-1, keepdims=True))
            p = (e / jnp.sum(e, axis=-1, keepdims=True)).astype(BF)
            total = total + jnp.dot(p, value * own, preferred_element_type=F32)
        mix_all[pl.ds(m, 1), i] = total.T.astype(BF)[None]
        hop(i, 0)
        if i == 0:
            fc1.relay()
            fc2.begin(fc2_ref.at[g])

    hop(0, 1)
    proj.relay()
    hop(1, 1)
    hop(0, 2)
    fc1.last()
    fc2.relay()
    hop(1, 2)
    proj.last()
    hop(0, 3)
    proj.finish()

    ff = fc1_ref.shape[2]
    share = tokens // nm
    k_rs = cp.slots(2 * (nm - 1))
    for i in range(images):
        if i:
            hop(i, 3)
        gate, shift, scale = piece(2, i), piece(3, i), piece(4, i)
        full = mix_all[:, i].reshape(width, tokens).T
        attn = dot_nt(full, proj_all[...].reshape(width, width))
        x1_ref[i] = attn

        @pl.loop(0, 4)
        def _(c):
            rows = pl.ds(pl.multiple_of(c * step, step), step)
            v = x_ref[i, rows, :].astype(F32) + gate * x1_ref[i, rows, :]
            x1_ref[i, rows, :] = v
            h_ref[i, rows, :] = (layer_norm(v) * (1.0 + scale) + shift).astype(BF)

        if i == 0:
            fc1.finish()

        @pl.loop(0, 2)
        def _(c):
            rows = pl.ds(pl.multiple_of(c * 2 * step, 2 * step), 2 * step)
            up = jnp.dot(
                h_ref[i, rows, :], fc1_all[...].reshape(width, ff), preferred_element_type=F32
            )
            gelu_ref[i, rows, :] = jax.nn.gelu(up, approximate=True).astype(BF)

        if i == 0:
            fc2.last()
            fc2.finish()
        rs_send[i] = dot_nt(gelu_ref[i], fc2_all[...].reshape(width, ff)).astype(BF)
        for b in range(1, nm):
            rows = pl.ds(pl.multiple_of(mpp(b) * share, share), share)
            cp.start(
                rs_send.at[i, rows],
                rs_recv.at[i, b - 1],
                k_rs + i * (nm - 1) + b - 1,
                {"mp": mpp(b)},
            )

    own_rows = pl.ds(pl.multiple_of(m * share, share), share)
    for b in range(1, nm):
        cp.arrived(fmod_all.at[mpp(-b)], k_fmod + b - 1, {"mp": mpp(-b)})
    fmods = functools.reduce(jnp.add, [fmod_all[b] for b in range(nm)])
    for i in range(images):
        mlp = rs_send[i, own_rows, :].astype(F32)
        for b in range(1, nm):
            cp.arrived(rs_recv.at[i, b - 1], k_rs + i * (nm - 1) + b - 1, {"mp": mpp(-b)})
            mlp = mlp + rs_recv[i, b - 1].astype(F32)
        v = x1_ref[i, own_rows, :] + piece(5, i) * mlp
        shift, scale = fmods[i : i + 1, :width], fmods[i : i + 1, width:]
        fin = (layer_norm(v) * (1.0 + scale) + shift).astype(BF)
        eps_ref[i] = dot_nt(fin, outw_ref[...])
    cp.drain()
    for cond, copy in held:

        @pl.when(cond)
        def _():
            copy.wait_send()


def on_device_kernel(
    x_arrive,
    cond_first,
    labels,
    step_ids,
    guidance,
    time_table,
    class_table,
    ada_weight,
    final_ada,
    qkv_weight,
    proj_weight,
    fc1_weight,
    fc2_weight,
    out_weight,
):
    nd, nm = lax.axis_size("dp"), lax.axis_size("mp")
    images, tokens, width = x_arrive.shape
    rows, quarter = qkv_weight.shape[1:]
    half = rows // 2
    ff = fc1_weight.shape[1]
    time_part = lax.dynamic_slice_in_dim(time_table, step_ids[0], 1, 0).astype(F32)
    class_part = lax.dynamic_slice_in_dim(class_table, labels[0], 1, 0).astype(F32)
    null_part = class_table[CLASSES].astype(F32)[None, :]
    first = cond_first[0] == 1
    act = jax.nn.silu(
        time_part
        + jnp.concatenate(
            [
                jnp.where(first, class_part, null_part),
                jnp.where(first, null_part, class_part),
            ]
        )
    ).astype(BF)
    act = jnp.pad(act.astype(F32), ((0, 8 - images), (0, 0)))
    fc1_in = fc1_weight.reshape(2, half, ff)
    fc2_in = fc2_weight.T.reshape(2, half, ff)
    copies = copy_count(nd, nm)
    vmem = pl.BlockSpec(memory_space=pltpu.VMEM)
    share = tokens // nm
    eps = pl.pallas_call(
        functools.partial(block_kernel, nd, nm, width // HEADS),
        out_shape=jax.ShapeDtypeStruct((images, share, out_weight.shape[1]), F32),
        in_specs=[vmem] * 9,
        out_specs=vmem,
        scratch_shapes=[
            pltpu.VMEM((nd,) + act.shape, F32),
            pltpu.VMEM((nd, images, ada_weight.shape[1]), F32),
            pltpu.VMEM((nd, nm, images, ada_weight.shape[1]), F32),
            pltpu.VMEM((images, final_ada.shape[1]), F32),
            pltpu.VMEM((nm, images, final_ada.shape[1]), F32),
            pltpu.VMEM((nd, 2, half, 3 * quarter), BF),
            pltpu.VMEM((2, half, quarter), BF),
            pltpu.VMEM((nm, half, quarter), BF),
            pltpu.VMEM((nd, 2, half, width), BF),
            pltpu.VMEM((nd, 2, half, ff), BF),
            pltpu.VMEM((nd, 2, half, ff), BF),
            pltpu.VMEM((images, tokens, width), BF),
            pltpu.VMEM((nm, images, quarter, tokens), BF),
            pltpu.VMEM((images, tokens, width), F32),
            pltpu.VMEM((images, tokens, ff), BF),
            pltpu.VMEM((images, tokens, width), BF),
            pltpu.VMEM((images, nm - 1, share, width), BF),
            pltpu.SemaphoreType.DMA((copies,)),
            pltpu.SemaphoreType.DMA((copies,)),
        ],
        compiler_params=pltpu.CompilerParams(
            collective_id=0, has_side_effects=True, vmem_limit_bytes=60 * 1024 * 1024
        ),
        name="dit_block",
    )(
        x_arrive,
        act,
        ada_weight,
        final_ada,
        qkv_weight,
        proj_weight,
        fc1_in,
        fc2_in,
        out_weight.T,
    )
    cond = jnp.where(first, eps[0], eps[1])
    uncond = jnp.where(first, eps[1], eps[0])
    return (uncond + guidance[0] * (cond - uncond)).reshape(1, share * out_weight.shape[1])


def solution(mesh):
    placed = (
        P(("group", "dp"), None, None),
        P(("group", "dp")),
        P(("group", "dp")),
        P(("group", "dp")),
        P(),
        P(None, "mp"),
        P(None, "mp"),
        P("mp", "dp"),
        P("mp", None),
        P(None, "dp", "mp"),
        P("mp", "dp"),
        P("dp", "mp"),
        P("mp", "dp"),
        P(),
    )
    def body(*args):
        rows = args[9].shape[1]
        fits = args[0].shape[0] == 2 and mesh.shape["group"] == 2 and rows % 32 == 0
        fits = fits and mesh.shape["dp"] == 4 and mesh.shape["mp"] == 4
        return on_device_kernel(*args) if fits else on_device(*args)

    return jax.shard_map(
        body, mesh=mesh, in_specs=placed, out_specs=P(("group", "dp"), "mp"), check_vma=False
    )
```
